32 devices in a mesh: groups: 2 (over y), gz: 8 (over z, x), ea: 2 (over core).
Axes of the slice: x: 2, y: 2, z: 4, core: 2. Of those that a mesh axis runs over, the one named last changes fastest.
Arguments:
- eigvec: bfloat16 [96, 3, 2, 16, 512], P('ea', None, None, ('groups', 'gz')), parts along dimension 3, may hold values from -3 to 3
- links: float32 [3, 3, 3, 2, 16, 512], P(None, None, None, None, ('groups', 'gz')), parts along dimension 4, may hold values from -1.8 to 1.8
- momentum: int32 [6], P('groups'), parts along dimension 0, may hold values from -2 to 2
- weights: int32 [6], P('groups'), parts along dimension 0, may hold values from 1 to 3
- spins: int32 [6, 2], P('groups'), parts along dimension 0, may hold values from 0 to 3
- peram: float32 [8, 4, 2, 96, 96], P('groups'), parts along dimension 0, may hold values from -0.4375 to 0.4375
Outputs:
- baryon_block: float32 [4, 96, 9216], P('groups', 'ea', 'gz'), parts along dimension 0
The draws below stay inside these ranges and needn't reach their ends.
There are 2 independent parts, one for each index of `groups`. The reference program is written for one: setup_inputs(seed, part) draws one part's arguments, and reference() takes and returns one part's arrays. A program takes and returns all parts, laid end to end along the dimension named above; each array names one. Nothing has to cross between parts.
All inputs are finite; a program needn't handle non-finite values.
Results may differ from the reference program's by a relative error of at most 0.0045.
Values may be sent and summed in bfloat16 or wider, within the bound.
No kernel may reach another device: no remote copies, remote signals or barrier semaphores. Data moves between devices by JAX's collectives and lax.ppermute only.
A program may use at most 64 MiB of HBM per device.

```python
import math
import jax
import jax.numpy as jnp
from jax import lax

NVEC = 96
LX = 32
LY = 16
NSPIN = 4
PLANE = 512
NZ = 8
VOLUME = 4096


def set_ends(values, stream_key, smallest, largest):
    place = [jax.random.randint(jax.random.fold_in(stream_key, axis), (), 0, length) for axis, length in enumerate(values.shape)]
    longest = values.shape.index(max(values.shape))
    neighbour = place[:longest] + [(place[longest] + 1) % values.shape[longest]] + place[longest + 1:]
    return values.at[tuple(place)].set(smallest).at[tuple(neighbour)].set(largest)


def levels(rng, dims, cuts, least, largest):
    loudness, own = 1.0, jax.random.fold_in(rng, 6)
    for axis_at, blocks in cuts:
        draws = jnp.exp(jax.random.uniform(jax.random.fold_in(own, axis_at), (blocks,), jnp.float32, least / len(cuts), largest / len(cuts)))
        loudness = loudness * jnp.repeat(draws, dims[axis_at] // blocks).reshape([-1 if axis == axis_at else 1 for axis in range(len(dims))])
    return loudness


def scatter_about(rng, shape, scale, limit, split=(), held_as=jnp.bfloat16):
    array = jax.random.normal(rng, shape, jnp.float32) * scale
    if len(split) > 0:
        array = levels(rng, shape, split, -0.22, 0.18) * array
    return jnp.clip(array, min=-limit, max=limit).astype(held_as)


def setup_inputs(seed: int = 0, part: int = 0) -> dict:
    arg_keys = jax.random.split(jax.random.key(seed), 7)
    part_keys = jax.random.split(jax.random.fold_in(arg_keys[6], part), 7)
    eigvec = scatter_about(part_keys[0], (NVEC, 3, 2, NZ, PLANE), 0.5, 3.0, ((0, 2), (3, 8)))
    links = scatter_about(part_keys[1], (3, 3, 3, 2, NZ, PLANE), 0.3, 1.8, ((4, 8),), jnp.float32)
    momentum = jax.random.randint(part_keys[2], (3,), -2, 3).astype(jnp.int32)
    weights = jax.random.randint(part_keys[3], (3,), 1, 4).astype(jnp.int32)
    spins = set_ends(jax.random.randint(part_keys[4], (3, 2), 0, 4), jax.random.fold_in(part_keys[4], 1), 0, 3).astype(jnp.int32)
    peram = scatter_about(part_keys[5], (NSPIN, NSPIN, 2, NVEC, NVEC), (2 * NVEC) ** -0.5, 0.4375, (), jnp.float32)
    return dict(eigvec=eigvec, links=links, momentum=momentum, weights=weights, spins=spins, peram=peram)


def link_apply(link, lattice_field):
    result_real = 0.0
    result_imaginary = 0.0
    for column_slot in range(3):
        gauge_link_real = link[None, :, column_slot, 0]
        gauge_link_imaginary = link[None, :, column_slot, 1]
        vector_real = lattice_field[:, None, column_slot, 0]
        vector_imaginary = lattice_field[:, None, column_slot, 1]
        result_real = result_real + gauge_link_real * vector_real - gauge_link_imaginary * vector_imaginary
        result_imaginary = result_imaginary + gauge_link_real * vector_imaginary + gauge_link_imaginary * vector_real
    return jnp.stack([result_real, result_imaginary], 2)

def adjoint_apply(link, lattice_field):
    result_real = 0.0
    result_imaginary = 0.0
    for column_slot in range(3):
        gauge_link_real = link[None, column_slot, :, 0]
        gauge_link_imaginary = link[None, column_slot, :, 1]
        vector_real = lattice_field[:, None, column_slot, 0]
        vector_imaginary = lattice_field[:, None, column_slot, 1]
        result_real = result_real + gauge_link_real * vector_real + gauge_link_imaginary * vector_imaginary
        result_imaginary = result_imaginary + gauge_link_real * vector_imaginary - gauge_link_imaginary * vector_real
    return jnp.stack([result_real, result_imaginary], 2)

def cross_parts(left_vec, right_vec):
    reals = []
    imags = []
    for first, second in ((1, 2), (2, 0), (0, 1)):
        ar = left_vec[:, :, first, 0]
        ai = left_vec[:, :, first, 1]
        br = left_vec[:, :, second, 0]
        bi = left_vec[:, :, second, 1]
        cr = right_vec[:, :, first, 0]
        ci = right_vec[:, :, first, 1]
        dr = right_vec[:, :, second, 0]
        di = right_vec[:, :, second, 1]
        reals.append(ar * dr - ai * di - (br * cr - bi * ci))
        imags.append(ar * di + ai * dr - (br * ci + bi * cr))
    return jnp.stack([jnp.stack(reals), jnp.stack(imags)])

def mode_product(lattice_field, block, form):
    high = lax.Precision.HIGHEST
    real_part = jnp.einsum(form, lattice_field[0], block[0], precision=high) - jnp.einsum(form, lattice_field[1], block[1], precision=high)
    imag_part = jnp.einsum(form, lattice_field[0], block[1], precision=high) + jnp.einsum(form, lattice_field[1], block[0], precision=high)
    return jnp.stack([real_part, imag_part])

def reference(eigvec, links, momentum, weights, spins, peram):
    vecf = eigvec.astype(jnp.float32)
    shape_full = vecf.shape[:4] + (LY, LX)
    grid = vecf.reshape(shape_full)
    linkgrid = links.reshape(links.shape[:5] + (LY, LX))
    axes_of = (5, 4, 3)
    disp = jnp.zeros(shape_full, jnp.float32)
    for direction in range(3):
        link = linkgrid[direction]
        ahead = jnp.roll(grid, -1, axes_of[direction])
        back = adjoint_apply(link, grid).astype(jnp.bfloat16)
        behind = jnp.roll(back, 1, axes_of[direction])
        behind = lax.optimization_barrier(behind).astype(jnp.float32)
        factor = weights[direction].astype(jnp.float32)
        disp = disp + factor * (link_apply(link, ahead) - behind)
    disp = disp.reshape(vecf.shape)
    sites = jnp.arange(PLANE, dtype=jnp.int32)
    xcoord = sites % LX
    ycoord = sites // LX
    zcoord = jnp.arange(NZ, dtype=jnp.int32)
    two_pi = 2.0 * math.pi
    inplane = (momentum[0] * xcoord).astype(jnp.float32) / LX + (momentum[1] * ycoord).astype(jnp.float32) / LY
    angle = two_pi * inplane[None, :] + two_pi * (momentum[2] * zcoord).astype(jnp.float32)[:, None] / NZ
    cosine = jnp.cos(angle)
    sine = jnp.sin(angle)
    phased_re = cosine * disp[:, :, 0] + sine * disp[:, :, 1]
    phased_im = cosine * disp[:, :, 1] - sine * disp[:, :, 0]
    phased = jnp.stack([phased_re, phased_im], 2).astype(jnp.bfloat16).astype(jnp.float32)
    high = lax.Precision.HIGHEST

    def plane_step(total, planes):
        vplane, dplane = planes
        wmat = cross_parts(vplane[:, None], vplane[None]).astype(jnp.bfloat16)
        wmat = lax.optimization_barrier(wmat).astype(jnp.float32)
        lre = dplane[:, :, 0]
        lim = dplane[:, :, 1]
        ere = jnp.einsum('aks,kbcs->abc', lre, wmat[0], precision=high) - jnp.einsum('aks,kbcs->abc', lim, wmat[1], precision=high)
        eim = jnp.einsum('aks,kbcs->abc', lre, wmat[1], precision=high) + jnp.einsum('aks,kbcs->abc', lim, wmat[0], precision=high)
        return (total + jnp.stack([ere, eim]), None)
    start = jnp.zeros((2, NVEC, NVEC, NVEC), jnp.float32)
    elemental, unused = lax.scan(plane_step, start, (jnp.moveaxis(vecf, 3, 0), jnp.moveaxis(phased, 3, 0)))
    elemental = elemental * (1.0 / math.sqrt(VOLUME))
    blocks = [peram[spins[q, 0], spins[q, 1]] for q in range(3)]
    result = mode_product(elemental, blocks[2], 'abc,cf->abf')
    result = mode_product(result, blocks[1], 'abc,be->aec')
    result = mode_product(result, blocks[0], 'abc,ad->dbc')
    return result.reshape(2, NVEC, NVEC * NVEC)
```

```python
import functools
import math

import jax
import jax.numpy as jnp
from jax import lax
from jax.experimental import pallas as pl
from jax.experimental.pallas import tpu as pltpu
from jax.sharding import PartitionSpec as P

LX = 32
LY = 16


F32 = jnp.float32
BF16 = jnp.bfloat16


def shift(array, axis, by):
    count = lax.axis_size(axis)
    return lax.ppermute(array, axis, [(i, (i + by) % count) for i in range(count)])


def link_mul(link, vec):
    out = []
    for row in range(3):
        re = im = 0.0
        for col in range(3):
            ur, ui = link(row, col, 0), link(row, col, 1)
            vr, vi = vec[2 * col], vec[2 * col + 1]
            re = re + ur * vr - ui * vi
            im = im + ur * vi + ui * vr
        out += [re, im]
    return out


def link_adj(link, vec):
    out = []
    for row in range(3):
        re = im = 0.0
        for col in range(3):
            ur, ui = link(col, row, 0), link(col, row, 1)
            vr, vi = vec[2 * col], vec[2 * col + 1]
            re = re + ur * vr + ui * vi
            im = im + ur * vi - ui * vr
        out += [re, im]
    return [x.astype(BF16).astype(F32) for x in out]


def stencil_kernel(weights, v_ref, up_ref, down_ref, link_ref, below_ref, trig_ref, out_ref):
    plane = v_ref.shape[2]
    rows = 16
    lane = lax.broadcasted_iota(jnp.int32, (1, plane), 1)
    xcoord = lane % LX

    def roll(a, by):
        return pltpu.roll(a, by % plane, 1)

    def from_dir(direction):
        def link(row, col, part):
            at = ((direction * 3 + row) * 3 + col) * 2 + part
            return link_ref[at : at + 1, :]

        return link

    def below(row, col, part):
        at = (row * 3 + col) * 2 + part
        return below_ref[at : at + 1, :]

    def body(step, carry):
        at = pl.ds(pl.multiple_of(step * rows, rows), rows)
        vec = [v_ref[i, at, :].astype(F32) for i in range(6)]
        disp = []
        ahead = [jnp.where(xcoord == LX - 1, roll(a, LX - 1), roll(a, -1)) for a in vec]
        back = link_adj(from_dir(0), vec)
        behind = [jnp.where(xcoord == 0, roll(a, 1 - LX), roll(a, 1)) for a in back]
        factor = weights[0].astype(F32)
        fore = link_mul(from_dir(0), ahead)
        disp = [factor * (f - b) for f, b in zip(fore, behind)]
        ahead = [roll(a, -LX) for a in vec]
        behind = [roll(a, LX) for a in link_adj(from_dir(1), vec)]
        factor = weights[1].astype(F32)
        fore = link_mul(from_dir(1), ahead)
        disp = [d + factor * (f - b) for d, f, b in zip(disp, fore, behind)]
        ahead = [up_ref[i, at, :].astype(F32) for i in range(6)]
        behind = link_adj(below, [down_ref[i, at, :].astype(F32) for i in range(6)])
        factor = weights[2].astype(F32)
        fore = link_mul(from_dir(2), ahead)
        disp = [d + factor * (f - b) for d, f, b in zip(disp, fore, behind)]
        cosine = trig_ref[0:1, :]
        sine = trig_ref[1:2, :]
        for k in range(3):
            re, im = disp[2 * k], disp[2 * k + 1]
            out_ref[2 * k, at, :] = (cosine * re + sine * im).astype(BF16)
            out_ref[2 * k + 1, at, :] = (cosine * im - sine * re).astype(BF16)
        return carry

    lax.fori_loop(0, v_ref.shape[1] // rows, body, 0)


def two_pass(mat, vec, swap):
    high = mat.astype(BF16)
    low = (mat - high.astype(F32)).astype(BF16)
    dims = (((0,), (0,)), ((), ()))
    if swap:
        return lax.dot_general(vec, high, dims, preferred_element_type=F32) + lax.dot_general(
            vec, low, dims, preferred_element_type=F32
        )
    return lax.dot_general(high, vec, dims, preferred_element_type=F32) + lax.dot_general(
        low, vec, dims, preferred_element_type=F32
    )


def modes_kernel(v_ref, t1_ref, t2_ref, t2i_ref, v1_ref, m_ref):
    plane = v_ref.shape[3]
    half = v_ref.shape[2]
    n = 2 * half
    for k in range(3):
        vk = jnp.concatenate([v_ref[h, 2 * k + r] for r in range(2) for h in range(2)], 0)
        one = two_pass(t1_ref[...], vk, False)
        v1_ref[:, 3 * k, :] = one[:n]
        v1_ref[:, 3 * k + 1, :] = one[n:]
        v1_ref[:, 3 * k + 2, :] = one[:n] + one[n:]
        m_ref[pl.ds(2 * k * plane, plane), :] = two_pass(t2_ref[...], vk, True).astype(BF16)
        m_ref[pl.ds((2 * k + 1) * plane, plane), :] = two_pass(t2i_ref[...], vk, True).astype(BF16)


def phi_kernel(phi_ref, t0_ref, out_ref):
    half = phi_ref.shape[2]
    for k in range(3):
        pk = jnp.concatenate([phi_ref[h, 2 * k + r] for r in range(2) for h in range(2)], 0)
        one = two_pass(t0_ref[...], pk, False)
        out_ref[3 * k] = one[:half]
        out_ref[3 * k + 1] = one[half:]
        out_ref[3 * k + 2] = one[:half] + one[half:]


def main_kernel(order, phi_ref, v1_ref, m_ref, out_ref, w_ref):
    block = out_ref.shape[1] * 2
    rows = phi_ref.shape[1]
    plane = phi_ref.shape[2]
    cols = m_ref.shape[1]
    base = order[pl.program_id(0)] * block
    lanes = 128

    def body(t, carry):
        for x in range(0, plane, lanes):
            at = pl.ds(x, lanes)
            v = [v1_ref[base + t, i : i + 1, at] for i in range(9)]
            for r in range(0, rows, 16):
                p = [phi_ref[i, r : r + 16, x : x + lanes] for i in range(9)]
                to = pl.ds(pl.multiple_of(t * rows + r, 16), 16)
                for k in range(3):
                    i, j = (k + 1) % 3, (k + 2) % 3
                    rr = p[3 * i] * v[3 * j] - p[3 * j] * v[3 * i]
                    ii = p[3 * i + 1] * v[3 * j + 1] - p[3 * j + 1] * v[3 * i + 1]
                    ss = p[3 * i + 2] * v[3 * j + 2] - p[3 * j + 2] * v[3 * i + 2]
                    w_ref[to, pl.ds(2 * k * plane + x, lanes)] = (rr - ii).astype(BF16)
                    w_ref[to, pl.ds((2 * k + 1) * plane + x, lanes)] = (ss - (rr + ii)).astype(BF16)
        return carry

    lax.fori_loop(0, block, body, 0)
    res = jnp.dot(w_ref[...], m_ref[...], preferred_element_type=F32)
    for t in range(block // 2):
        lo = res[2 * t * rows : (2 * t + 1) * rows]
        hi = res[(2 * t + 1) * rows : (2 * t + 2) * rows]
        out_ref[0, t] = jnp.concatenate([lo, hi], 1).astype(out_ref.dtype)


def sum_kernel(*refs):
    ins, out_ref = refs[:-1], refs[-1]
    pairs, rows, width = ins[0].shape
    n = width // 4
    for t in range(pairs):
        total = ins[0][t].astype(F32)
        for ref in ins[1:]:
            total = total + ref[t].astype(F32)
        for h in range(2):
            for r in range(2):
                at = (2 * h + r) * n
                to = (2 * t + h) * n
                out_ref[r, :, to : to + n] = total[:, at : at + n]


def mode_matrix(block):
    top = jnp.concatenate([block[0], block[1]], 1)
    bottom = jnp.concatenate([-block[1], block[0]], 1)
    return jnp.concatenate([top, bottom], 0)


def shards(eigvec, links, momentum, weights, spins, peram):
    half, plane = eigvec.shape[0], eigvec.shape[4]
    count = peram.shape[-1]
    slabs = lax.axis_size("gz")
    here = lax.axis_index("gz")
    core = lax.axis_index("ea")
    vec = eigvec.reshape(half, 6, plane).transpose(1, 0, 2)
    link = links.reshape(54, plane)
    upper = shift(vec, "gz", -1)
    lower = shift(vec, "gz", 1)
    below = shift(link[36:], "gz", 1)
    every = lax.all_gather(vec, "ea", axis=0)
    blocks = [peram[spins[q, 0], spins[q, 1]] for q in range(3)]
    t1 = mode_matrix(blocks[1])
    t2 = mode_matrix(blocks[2]) * (1.0 / math.sqrt(LX * LY * slabs))
    t2i = jnp.concatenate([-t2[:, count:], t2[:, :count]], 1)
    mine = lax.dynamic_slice_in_dim(blocks[0], core * half, half, 2)
    t0 = mode_matrix(mine)

    sites = jnp.arange(plane, dtype=jnp.int32)
    two_pi = 2.0 * math.pi
    inplane = (momentum[0] * (sites % LX)).astype(F32) / LX + (momentum[1] * (sites // LX)).astype(
        F32
    ) / LY
    angle = two_pi * inplane + two_pi * (momentum[2] * here).astype(F32) / slabs
    trig = jnp.stack([jnp.cos(angle), jnp.sin(angle)])

    smem = pl.BlockSpec(memory_space=pltpu.SMEM)
    vmem = pl.BlockSpec(memory_space=pltpu.VMEM)
    one, mat = pl.pallas_call(
        modes_kernel,
        out_shape=(
            jax.ShapeDtypeStruct((count, 9, plane), F32),
            jax.ShapeDtypeStruct((6 * plane, 2 * count), BF16),
        ),
        in_specs=[vmem] * 4,
        out_specs=(vmem, vmem),
        name="modes",
    )(every, t1, t2, t2i)
    phased = pl.pallas_call(
        stencil_kernel,
        out_shape=jax.ShapeDtypeStruct(vec.shape, BF16),
        in_specs=[smem] + [vmem] * 6,
        out_specs=vmem,
        name="stencil",
    )(weights, vec, upper, lower, link, below, trig)
    phases = lax.all_gather(phased, "ea", axis=0)
    phi = pl.pallas_call(
        phi_kernel,
        out_shape=jax.ShapeDtypeStruct((9, half, plane), F32),
        in_specs=[vmem] * 2,
        out_specs=vmem,
        name="phi",
    )(phases, t0)

    aligned = count % (2 * slabs) == 0
    parts = slabs if aligned else count // 8
    block = count // parts

    def products(order, dtype):
        number = order.shape[0]
        return pl.pallas_call(
            main_kernel,
            grid_spec=pltpu.PrefetchScalarGridSpec(
                num_scalar_prefetch=1,
                grid=(number,),
                in_specs=[vmem] * 3,
                out_specs=pl.BlockSpec(
                    (1, block // 2, half, 4 * count), lambda i, order: (i, 0, 0, 0)
                ),
                scratch_shapes=[pltpu.VMEM((block * half, 6 * plane), BF16)],
            ),
            out_shape=jax.ShapeDtypeStruct((number, block // 2, half, 4 * count), dtype),
            name="products",
        )(order, phi, one, mat)

    if not aligned:
        full = products(jnp.arange(parts, dtype=jnp.int32), F32)
        full = full.reshape(count // 2, half, 2, 2, count)
        full = full.transpose(3, 1, 0, 2, 4).reshape(2, half, count * count)
        return lax.psum_scatter(full, "gz", scatter_dimension=2, tiled=True)

    steps = list(range(1, slabs)) + [0]
    size = 2
    pieces = []
    for first in range(0, slabs, size):
        group = steps[first : first + size]
        order = (here + jnp.array(group, jnp.int32)) % slabs
        made = products(order.astype(jnp.int32), BF16)
        for at, step in enumerate(group):
            piece = made[at]
            pieces.append(shift(piece, "gz", step) if step else piece)
    return pl.pallas_call(
        sum_kernel,
        out_shape=jax.ShapeDtypeStruct((2, half, count * count // slabs), F32),
        in_specs=[vmem] * len(pieces),
        out_specs=vmem,
        name="total",
    )(*pieces)


def solution(mesh):
    in_specs = (
        P("ea", None, None, ("groups", "gz"), None),
        P(None, None, None, None, ("groups", "gz"), None),
        P("groups"),
        P("groups"),
        P("groups", None),
        P("groups", None, None, None, None),
    )
    out_specs = P("groups", "ea", "gz")
    return jax.shard_map(shards, mesh=mesh, in_specs=in_specs, out_specs=out_specs, check_vma=False)
```

```python
import functools
import math

import jax
import jax.numpy as jnp
from jax import lax
from jax.experimental import pallas as pl
from jax.experimental.pallas import tpu as pltpu
from jax.sharding import PartitionSpec as P

LX = 32
LY = 16


F32 = jnp.float32
BF16 = jnp.bfloat16


def shift(array, axis, by):
    count = lax.axis_size(axis)
    return lax.ppermute(array, axis, [(i, (i + by) % count) for i in range(count)])


def link_mul(link, vec):
    out = []
    for row in range(3):
        re = im = 0.0
        for col in range(3):
            ur, ui = link(row, col, 0), link(row, col, 1)
            vr, vi = vec[2 * col], vec[2 * col + 1]
            re = re + ur * vr - ui * vi
            im = im + ur * vi + ui * vr
        out += [re, im]
    return out


def link_adj(link, vec):
    out = []
    for row in range(3):
        re = im = 0.0
        for col in range(3):
            ur, ui = link(col, row, 0), link(col, row, 1)
            vr, vi = vec[2 * col], vec[2 * col + 1]
            re = re + ur * vr + ui * vi
            im = im + ur * vi - ui * vr
        out += [re, im]
    return [x.astype(BF16).astype(F32) for x in out]


def stencil_kernel(slabs, weights, momentum, here, v_ref, up_ref, down_ref, link_ref, below_ref, out_ref):
    plane = v_ref.shape[2]
    rows = 16
    lane = lax.broadcasted_iota(jnp.int32, (1, plane), 1)
    xcoord = lane % LX
    two_pi = 2.0 * math.pi
    inplane = (momentum[0] * xcoord).astype(F32) * (1.0 / LX) + (
        momentum[1] * (lane // LX)
    ).astype(F32) * (1.0 / LY)
    along = (momentum[2] * (lane * 0 + here[0])).astype(F32) * (1.0 / slabs)
    angle = two_pi * inplane + two_pi * along
    cosine = jnp.cos(angle)
    sine = jnp.sin(angle)

    def roll(a, by):
        return pltpu.roll(a, by % plane, 1)

    def from_dir(direction):
        def link(row, col, part):
            at = ((direction * 3 + row) * 3 + col) * 2 + part
            return link_ref[at : at + 1, :]

        return link

    def below(row, col, part):
        at = (row * 3 + col) * 2 + part
        return below_ref[at : at + 1, :]

    def body(step, carry):
        at = pl.ds(pl.multiple_of(step * rows, rows), rows)
        vec = [v_ref[i, at, :].astype(F32) for i in range(6)]
        disp = []
        ahead = [jnp.where(xcoord == LX - 1, roll(a, LX - 1), roll(a, -1)) for a in vec]
        back = link_adj(from_dir(0), vec)
        behind = [jnp.where(xcoord == 0, roll(a, 1 - LX), roll(a, 1)) for a in back]
        factor = weights[0].astype(F32)
        fore = link_mul(from_dir(0), ahead)
        disp = [factor * (f - b) for f, b in zip(fore, behind)]
        ahead = [roll(a, -LX) for a in vec]
        behind = [roll(a, LX) for a in link_adj(from_dir(1), vec)]
        factor = weights[1].astype(F32)
        fore = link_mul(from_dir(1), ahead)
        disp = [d + factor * (f - b) for d, f, b in zip(disp, fore, behind)]
        ahead = [up_ref[i, at, :].astype(F32) for i in range(6)]
        behind = link_adj(below, [down_ref[i, at, :].astype(F32) for i in range(6)])
        factor = weights[2].astype(F32)
        fore = link_mul(from_dir(2), ahead)
        disp = [d + factor * (f - b) for d, f, b in zip(disp, fore, behind)]
        for k in range(3):
            re, im = disp[2 * k], disp[2 * k + 1]
            out_ref[2 * k, at, :] = (cosine * re + sine * im).astype(BF16)
            out_ref[2 * k + 1, at, :] = (cosine * im - sine * re).astype(BF16)
        return carry

    lax.fori_loop(0, v_ref.shape[1] // rows, body, 0)


def two_pass(mat, vec, swap):
    high = mat.astype(BF16)
    low = (mat - high.astype(F32)).astype(BF16)
    dims = (((0,), (0,)), ((), ()))
    if swap:
        return lax.dot_general(vec, high, dims, preferred_element_type=F32) + lax.dot_general(
            vec, low, dims, preferred_element_type=F32
        )
    return lax.dot_general(high, vec, dims, preferred_element_type=F32) + lax.dot_general(
        low, vec, dims, preferred_element_type=F32
    )


def mode_matrix(re, im):
    top = jnp.concatenate([re, im], 1)
    bottom = jnp.concatenate([-im, re], 1)
    return jnp.concatenate([top, bottom], 0)


def modes_kernel(scale, spins, v_ref, b1_ref, b2_ref, v1_ref, m_ref):
    plane = v_ref.shape[3]
    half = v_ref.shape[2]
    n = 2 * half
    t1 = mode_matrix(b1_ref[0, 0, 0], b1_ref[0, 0, 1])
    re, im = b2_ref[0, 0, 0] * scale, b2_ref[0, 0, 1] * scale
    t2 = mode_matrix(re, im)
    t2i = mode_matrix(-im, re)
    for k in range(3):
        vk = jnp.concatenate([v_ref[h, 2 * k + r] for r in range(2) for h in range(2)], 0)
        one = two_pass(t1, vk, False)
        v1_ref[:, 3 * k, :] = one[:n]
        v1_ref[:, 3 * k + 1, :] = one[n:]
        v1_ref[:, 3 * k + 2, :] = one[:n] + one[n:]
        m_ref[pl.ds(2 * k * plane, plane), :] = two_pass(t2, vk, True).astype(BF16)
        m_ref[pl.ds((2 * k + 1) * plane, plane), :] = two_pass(t2i, vk, True).astype(BF16)


def phi_kernel(spins, core, phi_ref, b0_ref, out_ref):
    half = phi_ref.shape[2]
    t0 = mode_matrix(b0_ref[0, 0, 0], b0_ref[0, 0, 1])
    for k in range(3):
        pk = jnp.concatenate([phi_ref[h, 2 * k + r] for r in range(2) for h in range(2)], 0)
        one = two_pass(t0, pk, False)
        first = core[0] == 0
        re = jnp.where(first, one[:half], one[half : 2 * half])
        im = jnp.where(first, one[2 * half : 3 * half], one[3 * half :])
        out_ref[3 * k] = re
        out_ref[3 * k + 1] = im
        out_ref[3 * k + 2] = re + im


def main_kernel(order, phi_ref, v1_ref, m_ref, *refs):
    outs, w_ref = refs[:-1], refs[-1]
    block = outs[0].shape[0] * 2
    rows = phi_ref.shape[1]
    plane = phi_ref.shape[2]
    lanes = 128
    for at_out, out_ref in enumerate(outs):
        base = order[at_out] * block

        def body(t, carry):
            for x in range(0, plane, lanes):
                at = pl.ds(x, lanes)
                v = [v1_ref[base + t, i : i + 1, at] for i in range(9)]
                for r in range(0, rows, 16):
                    p = [phi_ref[i, r : r + 16, x : x + lanes] for i in range(9)]
                    to = pl.ds(pl.multiple_of(t * rows + r, 16), 16)
                    for k in range(3):
                        i, j = (k + 1) % 3, (k + 2) % 3
                        rr = p[3 * i] * v[3 * j] - p[3 * j] * v[3 * i]
                        ii = p[3 * i + 1] * v[3 * j + 1] - p[3 * j + 1] * v[3 * i + 1]
                        ss = p[3 * i + 2] * v[3 * j + 2] - p[3 * j + 2] * v[3 * i + 2]
                        w_ref[to, pl.ds(2 * k * plane + x, lanes)] = (rr - ii).astype(BF16)
                        w_ref[to, pl.ds((2 * k + 1) * plane + x, lanes)] = (
                            ss - (rr + ii)
                        ).astype(BF16)
            return carry

        lax.fori_loop(0, block, body, 0)
        res = jnp.dot(w_ref[...], m_ref[...], preferred_element_type=F32)
        for t in range(block // 2):
            lo = res[2 * t * rows : (2 * t + 1) * rows]
            hi = res[(2 * t + 1) * rows : (2 * t + 2) * rows]
            out_ref[t] = jnp.concatenate([lo, hi], 1).astype(out_ref.dtype)


def sum_kernel(*refs):
    ins, out_ref = refs[:-1], refs[-1]
    pairs, rows, width = ins[0].shape
    n = width // 4
    for t in range(pairs):
        total = ins[0][t].astype(F32)
        for ref in ins[1:]:
            total = total + ref[t].astype(F32)
        for h in range(2):
            for r in range(2):
                at = (2 * h + r) * n
                to = (2 * t + h) * n
                out_ref[r, :, to : to + n] = total[:, at : at + n]


def shards(eigvec, links, momentum, weights, spins, peram):
    half, plane = eigvec.shape[0], eigvec.shape[4]
    count = peram.shape[-1]
    slabs = lax.axis_size("gz")
    here = lax.axis_index("gz")
    core = lax.axis_index("ea")
    vec = eigvec.reshape(half, 6, plane).transpose(1, 0, 2)
    link = links.reshape(54, plane)
    upper = shift(vec, "gz", -1)
    lower = shift(vec, "gz", 1)
    below = shift(link[36:], "gz", 1)
    every = lax.all_gather(vec, "ea", axis=0)

    smem = pl.BlockSpec(memory_space=pltpu.SMEM)
    vmem = pl.BlockSpec(memory_space=pltpu.VMEM)

    def chosen(q):
        return pl.BlockSpec(
            (1, 1, 2, count, count), lambda i, spins, *_: (spins[q, 0], spins[q, 1], 0, 0, 0)
        )

    one, mat = pl.pallas_call(
        functools.partial(modes_kernel, 1.0 / math.sqrt(LX * LY * slabs)),
        grid_spec=pltpu.PrefetchScalarGridSpec(
            num_scalar_prefetch=1,
            grid=(1,),
            in_specs=[vmem, chosen(1), chosen(2)],
            out_specs=(vmem, vmem),
        ),
        out_shape=(
            jax.ShapeDtypeStruct((count, 9, plane), F32),
            jax.ShapeDtypeStruct((6 * plane, 2 * count), BF16),
        ),
        name="modes",
    )(spins, every, peram, peram)
    phased = pl.pallas_call(
        functools.partial(stencil_kernel, slabs),
        out_shape=jax.ShapeDtypeStruct(vec.shape, BF16),
        in_specs=[smem] * 3 + [vmem] * 5,
        out_specs=vmem,
        name="stencil",
    )(weights, momentum, here.reshape(1), vec, upper, lower, link, below)
    phases = lax.all_gather(phased, "ea", axis=0)
    phi = pl.pallas_call(
        phi_kernel,
        grid_spec=pltpu.PrefetchScalarGridSpec(
            num_scalar_prefetch=2,
            grid=(1,),
            in_specs=[vmem, chosen(0)],
            out_specs=vmem,
        ),
        out_shape=jax.ShapeDtypeStruct((9, half, plane), F32),
        name="phi",
    )(spins, core.reshape(1), phases, peram)

    aligned = slabs % 2 == 0 and count % (2 * slabs) == 0
    block = count // slabs if aligned else 8

    def products(order, dtypes):
        return pl.pallas_call(
            main_kernel,
            in_specs=[smem] + [vmem] * 3,
            out_specs=[vmem] * len(dtypes),
            scratch_shapes=[pltpu.VMEM((block * half, 6 * plane), BF16)],
            out_shape=[
                jax.ShapeDtypeStruct((block // 2, half, 4 * count), dtype) for dtype in dtypes
            ],
            name="products",
        )(jnp.stack(order).astype(jnp.int32), phi, one, mat)

    if not aligned:
        full = [products([jnp.int32(i)], [F32])[0] for i in range(count // block)]
        full = jnp.concatenate(full, 0).reshape(count // 2, half, 2, 2, count)
        full = full.transpose(3, 1, 0, 2, 4).reshape(2, half, count * count)
        return lax.psum_scatter(full, "gz", scatter_dimension=2, tiled=True)

    pairs = slabs // 2
    swap = [(i, i ^ 1) for i in range(slabs)]
    steps = sorted(range(1, pairs), key=lambda s: -min(s, pairs - s)) + [0]
    pieces = []
    for step in steps:
        target = (here // 2 + step) % pairs * 2
        away, kept = products([target + (1 - here % 2), target + here % 2], [BF16, F32])
        got = lax.ppermute(away, "gz", swap)
        if step:
            both = (kept + got.astype(F32)).astype(BF16)
            pieces.append(shift(both, "gz", 2 * step))
        else:
            pieces += [kept, got]
    return pl.pallas_call(
        sum_kernel,
        out_shape=jax.ShapeDtypeStruct((2, half, count * count // slabs), F32),
        in_specs=[vmem] * len(pieces),
        out_specs=vmem,
        name="total",
    )(*pieces)


def solution(mesh):
    in_specs = (
        P("ea", None, None, ("groups", "gz"), None),
        P(None, None, None, None, ("groups", "gz"), None),
        P("groups"),
        P("groups"),
        P("groups", None),
        P("groups", None, None, None, None),
    )
    out_specs = P("groups", "ea", "gz")
    return jax.shard_map(shards, mesh=mesh, in_specs=in_specs, out_specs=out_specs, check_vma=False)
```

```python
import functools
import math

import jax
import jax.numpy as jnp
from jax import lax
from jax.experimental import pallas as pl
from jax.experimental.pallas import tpu as pltpu
from jax.sharding import PartitionSpec as P

LX = 32
LY = 16


F32 = jnp.float32
BF16 = jnp.bfloat16


def shift(array, axis, by):
    count = lax.axis_size(axis)
    return lax.ppermute(array, axis, [(i, (i + by) % count) for i in range(count)])


def link_mul(link, vec):
    out = []
    for row in range(3):
        re = im = 0.0
        for col in range(3):
            ur, ui = link(row, col, 0), link(row, col, 1)
            vr, vi = vec[2 * col], vec[2 * col + 1]
            re = re + ur * vr - ui * vi
            im = im + ur * vi + ui * vr
        out += [re, im]
    return out


def link_adj(link, vec):
    out = []
    for row in range(3):
        re = im = 0.0
        for col in range(3):
            ur, ui = link(col, row, 0), link(col, row, 1)
            vr, vi = vec[2 * col], vec[2 * col + 1]
            re = re + ur * vr + ui * vi
            im = im + ur * vi - ui * vr
        out += [re, im]
    return [x.astype(BF16).astype(F32) for x in out]


def stencil_kernel(slabs, weights, momentum, here, v_ref, up_ref, down_ref, link_ref, below_ref, out_ref):
    plane = v_ref.shape[2]
    rows = 16
    lane = lax.broadcasted_iota(jnp.int32, (1, plane), 1)
    xcoord = lane % LX
    two_pi = 2.0 * math.pi
    inplane = (momentum[0] * xcoord).astype(F32) * (1.0 / LX) + (
        momentum[1] * (lane // LX)
    ).astype(F32) * (1.0 / LY)
    along = (momentum[2] * (lane * 0 + here[0])).astype(F32) * (1.0 / slabs)
    angle = two_pi * inplane + two_pi * along
    cosine = jnp.cos(angle)
    sine = jnp.sin(angle)

    def roll(a, by):
        return pltpu.roll(a, by % plane, 1)

    def from_dir(direction):
        def link(row, col, part):
            at = ((direction * 3 + row) * 3 + col) * 2 + part
            return link_ref[at : at + 1, :]

        return link

    def below(row, col, part):
        at = (row * 3 + col) * 2 + part
        return below_ref[at : at + 1, :]

    def body(step, carry):
        at = pl.ds(pl.multiple_of(step * rows, rows), rows)
        vec = [v_ref[i, at, :].astype(F32) for i in range(6)]
        disp = []
        ahead = [jnp.where(xcoord == LX - 1, roll(a, LX - 1), roll(a, -1)) for a in vec]
        back = link_adj(from_dir(0), vec)
        behind = [jnp.where(xcoord == 0, roll(a, 1 - LX), roll(a, 1)) for a in back]
        factor = weights[0].astype(F32)
        fore = link_mul(from_dir(0), ahead)
        disp = [factor * (f - b) for f, b in zip(fore, behind)]
        ahead = [roll(a, -LX) for a in vec]
        behind = [roll(a, LX) for a in link_adj(from_dir(1), vec)]
        factor = weights[1].astype(F32)
        fore = link_mul(from_dir(1), ahead)
        disp = [d + factor * (f - b) for d, f, b in zip(disp, fore, behind)]
        ahead = [up_ref[i, at, :].astype(F32) for i in range(6)]
        behind = link_adj(below, [down_ref[i, at, :].astype(F32) for i in range(6)])
        factor = weights[2].astype(F32)
        fore = link_mul(from_dir(2), ahead)
        disp = [d + factor * (f - b) for d, f, b in zip(disp, fore, behind)]
        for k in range(3):
            re, im = disp[2 * k], disp[2 * k + 1]
            out_ref[2 * k, at, :] = (cosine * re + sine * im).astype(BF16)
            out_ref[2 * k + 1, at, :] = (cosine * im - sine * re).astype(BF16)
        return carry

    lax.fori_loop(0, v_ref.shape[1] // rows, body, 0)


def two_pass(mat, vec, swap):
    high = mat.astype(BF16)
    low = (mat - high.astype(F32)).astype(BF16)
    dims = (((0,), (0,)), ((), ()))
    if swap:
        return lax.dot_general(vec, high, dims, preferred_element_type=F32) + lax.dot_general(
            vec, low, dims, preferred_element_type=F32
        )
    return lax.dot_general(high, vec, dims, preferred_element_type=F32) + lax.dot_general(
        low, vec, dims, preferred_element_type=F32
    )


def mode_matrix(re, im):
    top = jnp.concatenate([re, im], 1)
    bottom = jnp.concatenate([-im, re], 1)
    return jnp.concatenate([top, bottom], 0)


def modes_kernel(scale, spins, v_ref, b1_ref, b2_ref, v1_ref, m_ref):
    plane = v_ref.shape[3]
    half = v_ref.shape[2]
    n = 2 * half
    t1 = mode_matrix(b1_ref[0, 0, 0], b1_ref[0, 0, 1])
    re, im = b2_ref[0, 0, 0] * scale, b2_ref[0, 0, 1] * scale
    t2 = mode_matrix(re, im)
    t2i = mode_matrix(-im, re)
    for k in range(3):
        vk = jnp.concatenate([v_ref[h, 2 * k + r] for r in range(2) for h in range(2)], 0)
        one = two_pass(t1, vk, False)
        v1_ref[:, 3 * k, :] = one[:n]
        v1_ref[:, 3 * k + 1, :] = one[n:]
        v1_ref[:, 3 * k + 2, :] = one[:n] + one[n:]
        m_ref[pl.ds(2 * k * plane, plane), :] = two_pass(t2, vk, True).astype(BF16)
        m_ref[pl.ds((2 * k + 1) * plane, plane), :] = two_pass(t2i, vk, True).astype(BF16)


def phi_kernel(spins, core, phi_ref, b0_ref, out_ref):
    half = phi_ref.shape[2]
    t0 = mode_matrix(b0_ref[0, 0, 0], b0_ref[0, 0, 1])
    for k in range(3):
        pk = jnp.concatenate([phi_ref[h, 2 * k + r] for r in range(2) for h in range(2)], 0)
        one = two_pass(t0, pk, False)
        first = core[0] == 0
        re = jnp.where(first, one[:half], one[half : 2 * half])
        im = jnp.where(first, one[2 * half : 3 * half], one[3 * half :])
        out_ref[3 * k] = re
        out_ref[3 * k + 1] = im
        out_ref[3 * k + 2] = re + im


def main_kernel(count, order, phi_ref, v1_ref, m_ref, *refs):
    outs, w_ref = refs[-1 - count : -1], refs[-1]
    block = outs[0].shape[0] * 2
    rows = phi_ref.shape[1]
    plane = phi_ref.shape[2]
    lanes = 128
    for at_out, out_ref in enumerate(outs):
        base = order[at_out] * block

        def body(t, carry):
            for x in range(0, plane, lanes):
                at = pl.ds(x, lanes)
                v = [v1_ref[base + t, i : i + 1, at] for i in range(9)]
                for r in range(0, rows, 16):
                    p = [phi_ref[i, r : r + 16, x : x + lanes] for i in range(9)]
                    to = pl.ds(pl.multiple_of(t * rows + r, 16), 16)
                    for k in range(3):
                        i, j = (k + 1) % 3, (k + 2) % 3
                        rr = p[3 * i] * v[3 * j] - p[3 * j] * v[3 * i]
                        ii = p[3 * i + 1] * v[3 * j + 1] - p[3 * j + 1] * v[3 * i + 1]
                        ss = p[3 * i + 2] * v[3 * j + 2] - p[3 * j + 2] * v[3 * i + 2]
                        w_ref[to, pl.ds(2 * k * plane + x, lanes)] = (rr - ii).astype(BF16)
                        w_ref[to, pl.ds((2 * k + 1) * plane + x, lanes)] = (
                            ss - (rr + ii)
                        ).astype(BF16)
            return carry

        lax.fori_loop(0, block, body, 0)
        res = jnp.dot(w_ref[...], m_ref[...], preferred_element_type=F32)
        for t in range(block // 2):
            lo = res[2 * t * rows : (2 * t + 1) * rows]
            hi = res[(2 * t + 1) * rows : (2 * t + 2) * rows]
            out_ref[t] = jnp.concatenate([lo, hi], 1).astype(out_ref.dtype)


def sum_kernel(*refs):
    ins, out_ref = refs[:-1], refs[-1]
    pairs, rows, width = ins[0].shape
    n = width // 4
    for t in range(pairs):
        total = ins[0][t].astype(F32)
        for ref in ins[1:]:
            total = total + ref[t].astype(F32)
        for h in range(2):
            for r in range(2):
                at = (2 * h + r) * n
                to = (2 * t + h) * n
                out_ref[r, :, to : to + n] = total[:, at : at + n]


def shards(eigvec, links, momentum, weights, spins, peram):
    half, plane = eigvec.shape[0], eigvec.shape[4]
    count = peram.shape[-1]
    slabs = lax.axis_size("gz")
    here = lax.axis_index("gz")
    core = lax.axis_index("ea")
    vec = eigvec.reshape(half, 6, plane).transpose(1, 0, 2)
    link = links.reshape(54, plane)
    upper = shift(vec, "gz", -1)
    lower = shift(vec, "gz", 1)
    below = shift(link[36:], "gz", 1)
    every = lax.all_gather(vec, "ea", axis=0)

    smem = pl.BlockSpec(memory_space=pltpu.SMEM)
    vmem = pl.BlockSpec(memory_space=pltpu.VMEM)

    def chosen(q):
        return pl.BlockSpec(
            (1, 1, 2, count, count), lambda i, spins, *_: (spins[q, 0], spins[q, 1], 0, 0, 0)
        )

    one, mat = pl.pallas_call(
        functools.partial(modes_kernel, 1.0 / math.sqrt(LX * LY * slabs)),
        grid_spec=pltpu.PrefetchScalarGridSpec(
            num_scalar_prefetch=1,
            grid=(1,),
            in_specs=[vmem, chosen(1), chosen(2)],
            out_specs=(vmem, vmem),
        ),
        out_shape=(
            jax.ShapeDtypeStruct((count, 9, plane), F32),
            jax.ShapeDtypeStruct((6 * plane, 2 * count), BF16),
        ),
        name="modes",
    )(spins, every, peram, peram)
    phased = pl.pallas_call(
        functools.partial(stencil_kernel, slabs),
        out_shape=jax.ShapeDtypeStruct(vec.shape, BF16),
        in_specs=[smem] * 3 + [vmem] * 5,
        out_specs=vmem,
        name="stencil",
    )(weights, momentum, here.reshape(1), vec, upper, lower, link, below)
    phases = lax.all_gather(phased, "ea", axis=0)
    phi = pl.pallas_call(
        phi_kernel,
        grid_spec=pltpu.PrefetchScalarGridSpec(
            num_scalar_prefetch=2,
            grid=(1,),
            in_specs=[vmem, chosen(0)],
            out_specs=vmem,
        ),
        out_shape=jax.ShapeDtypeStruct((9, half, plane), F32),
        name="phi",
    )(spins, core.reshape(1), phases, peram)

    aligned = slabs % 2 == 0 and count % (2 * slabs) == 0
    block = count // slabs if aligned else 8

    def products(order, dtypes, after=()):
        return pl.pallas_call(
            functools.partial(main_kernel, len(dtypes)),
            in_specs=[smem] + [vmem] * 3 + [pl.BlockSpec(memory_space=pl.ANY)] * len(after),
            out_specs=[vmem] * len(dtypes),
            scratch_shapes=[pltpu.VMEM((block * half, 6 * plane), BF16)],
            out_shape=[
                jax.ShapeDtypeStruct((block // 2, half, 4 * count), dtype) for dtype in dtypes
            ],
            name="products",
        )(jnp.stack(order).astype(jnp.int32), phi, one, mat, *after)

    if not aligned:
        full = [products([jnp.int32(i)], [F32])[0] for i in range(count // block)]
        full = jnp.concatenate(full, 0).reshape(count // 2, half, 2, 2, count)
        full = full.transpose(3, 1, 0, 2, 4).reshape(2, half, count * count)
        return lax.psum_scatter(full, "gz", scatter_dimension=2, tiled=True)

    pairs = slabs // 2
    swap = [(i, i ^ 1) for i in range(slabs)]
    steps = sorted(range(1, pairs), key=lambda s: -min(s, pairs - s)) + [0]
    pieces, waiting, ready = [], [], []

    def add():
        step, kept, got = waiting.pop(0)
        both = (kept + got.astype(F32)).astype(BF16)
        pieces.append(shift(both, "gz", 2 * step))
        ready[:] = [both]

    for step in steps:
        target = (here // 2 + step) % pairs * 2
        orders = target + (1 - here % 2), target + here % 2
        if len(waiting) > 1 or (waiting and not step):
            add()
        if step:
            away, kept = products(orders, [BF16, F32], ready)
            waiting.append((step, kept, lax.ppermute(away, "gz", swap)))
        else:
            (away,) = products(orders[:1], [BF16], ready)
            got = lax.ppermute(away, "gz", swap)
            while waiting:
                add()
            (kept,) = products(orders[1:], [F32], ready)
            pieces += [kept, got]
    return pl.pallas_call(
        sum_kernel,
        out_shape=jax.ShapeDtypeStruct((2, half, count * count // slabs), F32),
        in_specs=[vmem] * len(pieces),
        out_specs=vmem,
        name="total",
    )(*pieces)


def solution(mesh):
    in_specs = (
        P("ea", None, None, ("groups", "gz"), None),
        P(None, None, None, None, ("groups", "gz"), None),
        P("groups"),
        P("groups"),
        P("groups", None),
        P("groups", None, None, None, None),
    )
    out_specs = P("groups", "ea", "gz")
    return jax.shard_map(shards, mesh=mesh, in_specs=in_specs, out_specs=out_specs, check_vma=False)
```
